32 devices in a mesh: req: 8 (over y, x, core), head: 4 (over z).
Axes of the slice: x: 2, y: 2, z: 4, core: 2. Of those that a mesh axis runs over, the one named last changes fastest.
Arguments:
- queries: bfloat16 [128, 64, 128], P('req', 'head'), may hold values from -6 to 6
- k_codes: bfloat16 [8192, 16, 8, 128], P('req', None, 'head'), may hold values from -6 to 6
- value_quantized_codes: bfloat16 [8192, 16, 8, 128], P('req', None, 'head'), may hold values from -6 to 6
- key_page_scale: float32 [8192, 8], P('req', 'head'), may hold values from 0.5 to 2
- value_page_scale: float32 [8192, 8], P('req', 'head'), may hold values from 4 to 16
- lengths: int32 [128], P('req'), may hold values from 1 to 2032
- page_table: int32 [128, 128], P('req'), may hold values from -1 to 8191, as said below
- out_weight: bfloat16 [8192, 8192], P('head', 'req'), may hold values from -0.0625 to 0.0625
Outputs:
- attn_out: bfloat16 [128, 8192], P(None, ('req', 'head'))
The draws below stay inside these ranges and needn't reach their ends.
Inputs may be any that keep to these rules, and one draw needn't show every extreme that they name: `page_table`: entries j below ceil(lengths[r] / 16) name pool pages; all such entries of all requests together name every pool page exactly once. Entries beyond are -1.
All inputs are finite; a program needn't handle non-finite values.
Results may differ from the reference program's by a relative error of at most 0.02.
Values may be sent and summed in bfloat16 or wider, within the bound.
A program may use at most 128 MiB of HBM per device.

```python
import math
import jax
import jax.numpy as jnp
from jax import lax

QUERY_HEADS = 64
KEY_VALUE_HEADS = 8
HEAD_DIMENSION = 128
DMODEL = 8192
PAGE_TOKENS = 16
MAXP = 128
R_DEV = 16
REQS = 128
POOL_PAGES = 8192
N_REQ = 8


def page_layout(key):
    half_count = REQS // 2
    middle = MAXP // 2
    sign_dev = 2 * jax.random.randint(jax.random.fold_in(key, 1), (N_REQ // 2,), 0, 2) - 1
    shift = jax.random.randint(jax.random.fold_in(key, 2), (half_count,), 0, middle)
    selected_pages = jax.random.randint(jax.random.fold_in(key, 3), (), 0, half_count)
    shift = shift.at[selected_pages].set(middle - 1)
    owner_dev = jnp.arange(half_count, dtype=jnp.int32) // R_DEV
    turned = sign_dev[owner_dev] * shift
    page_count = jnp.concatenate([middle + turned, middle - turned]).astype(jnp.int32)
    remainder = jax.random.randint(jax.random.fold_in(key, 4), (REQS,), 1, PAGE_TOKENS + 1)
    longest = jnp.where(sign_dev[selected_pages // R_DEV] > 0, selected_pages, selected_pages + half_count)
    remainder = remainder.at[longest].set(PAGE_TOKENS)
    lengths = ((page_count - 1) * PAGE_TOKENS + remainder).astype(jnp.int32)
    shuffled = jax.random.permutation(jax.random.fold_in(key, 5), POOL_PAGES).astype(jnp.int32)
    starts = jnp.cumsum(page_count) - page_count
    entry = jnp.arange(MAXP, dtype=jnp.int32)[None, :]
    slot = jnp.clip(starts[:, None] + entry, 0, POOL_PAGES - 1)
    table = jnp.where(entry < page_count[:, None], shuffled[slot], -1).astype(jnp.int32)
    return (lengths, table)


def draw_lengths(key, part):
    return page_layout(jax.random.fold_in(key, 11))[0]


def draw_page_table(key, part):
    return page_layout(jax.random.fold_in(key, 11))[1]


def draw_queries(key, part):
    value_rows = jnp.clip(jax.random.normal(jax.random.fold_in(key, 21), (REQS, QUERY_HEADS, HEAD_DIMENSION), jnp.float32), -6.0, 6.0)
    return value_rows.astype(jnp.bfloat16)


def draw_k_codes(key, part):
    value_rows = jnp.clip(jax.random.normal(jax.random.fold_in(key, 31), (POOL_PAGES, PAGE_TOKENS, KEY_VALUE_HEADS, HEAD_DIMENSION), jnp.float32), -6.0, 6.0)
    return value_rows.astype(jnp.bfloat16)


def steps_of(rng, extent, split, smallest, high):
    level = 1.0
    for dim, parts in split:
        draws = jax.random.uniform(jax.random.fold_in(jax.random.fold_in(rng, 6), dim), (parts,), jnp.float32, smallest / len(split), high / len(split))
        level = level * jnp.repeat(jnp.exp(draws), extent[dim] // parts).reshape((-1,) + (1,) * (len(extent) - 1 - dim))
    return level


def normal_values(key, extent, width, reach, shards=(), held_as=jnp.bfloat16):
    level = steps_of(key, extent, shards, -0.22, 0.18) if shards else 1.0
    array = jax.random.normal(key, extent, jnp.float32) * width * level
    return jnp.minimum(jnp.maximum(array, -reach), reach).astype(held_as)


def setup_inputs(seed: int = 0) -> dict:
    arg_keys = jax.random.split(jax.random.key(seed), 9)
    queries = draw_queries(jax.random.fold_in(arg_keys[8], 71), 0)
    k_codes = draw_k_codes(jax.random.fold_in(arg_keys[8], 71), 0)
    value_quantized_codes = normal_values(arg_keys[2], (POOL_PAGES, PAGE_TOKENS, KEY_VALUE_HEADS, HEAD_DIMENSION), 1.0, 6.0, ((0, 8), (2, 4)))
    key_page_scale = jnp.clip(jnp.exp(math.log(2.0) - 1.3862944 * jax.random.uniform(arg_keys[3], (POOL_PAGES, KEY_VALUE_HEADS), jnp.float32) ** steps_of(arg_keys[3], (POOL_PAGES, KEY_VALUE_HEADS), ((0, 8), (1, 4)), -0.2, 0.2)), 0.5, 2.0)
    value_page_scale = jnp.clip(jnp.exp(math.log(16.0) - 1.3862944 * jax.random.uniform(arg_keys[4], (POOL_PAGES, KEY_VALUE_HEADS), jnp.float32) ** steps_of(arg_keys[4], (POOL_PAGES, KEY_VALUE_HEADS), ((0, 8), (1, 4)), -0.2, 0.2)), 4.0, 16.0)
    lengths = draw_lengths(jax.random.fold_in(arg_keys[8], 71), 0)
    page_table = draw_page_table(jax.random.fold_in(arg_keys[8], 71), 0)
    out_weight = normal_values(arg_keys[7], (QUERY_HEADS * HEAD_DIMENSION, DMODEL), (QUERY_HEADS * HEAD_DIMENSION) ** -0.5, 0.0625, ((0, 4), (1, 8)))
    return {"queries": queries, "k_codes": k_codes, "value_quantized_codes": value_quantized_codes, "key_page_scale": key_page_scale, "value_page_scale": value_page_scale, "lengths": lengths, "page_table": page_table, "out_weight": out_weight}


floor_score = -1e+30

def reference(queries, k_codes, value_quantized_codes, key_page_scale, value_page_scale, lengths, page_table, out_weight):
    query_group_count = QUERY_HEADS // KEY_VALUE_HEADS

    def per_request(inputs_row):
        query_vector, length_row, table_row = inputs_row
        page_ids = jnp.maximum(table_row, 0).astype(jnp.int32)
        keys = k_codes[page_ids].astype(jnp.float32)
        value_rows = value_quantized_codes[page_ids].astype(jnp.float32)
        query_float = query_vector.astype(jnp.float32).reshape(KEY_VALUE_HEADS, query_group_count, HEAD_DIMENSION)
        scores = jnp.einsum('kgd,ptkd->pkgt', query_float, keys)
        scores = scores * (key_page_scale[page_ids][:, :, None, None] / math.sqrt(HEAD_DIMENSION))
        position = jnp.arange(MAXP, dtype=jnp.int32)[:, None] * PAGE_TOKENS + jnp.arange(PAGE_TOKENS, dtype=jnp.int32)[None, :]
        is_live = (position < length_row)[:, None, None, :]
        page_max = lax.optimization_barrier(jnp.max(jnp.where(is_live, scores, floor_score), axis=-1))
        weights = jnp.where(is_live, jnp.exp(scores - page_max[..., None]), 0.0)
        weights = lax.optimization_barrier(weights.astype(jnp.bfloat16)).astype(jnp.float32)
        page_sum = lax.optimization_barrier(jnp.sum(weights, axis=-1))
        page_out = jnp.einsum('pkgt,ptkd->pkgd', weights, value_rows) * value_page_scale[page_ids][:, :, None, None]
        peak = lax.optimization_barrier(jnp.max(page_max, axis=0))
        factor = jnp.exp(page_max - peak)
        numerator = lax.optimization_barrier(jnp.sum(page_out * factor[..., None], axis=0))
        denominator = lax.optimization_barrier(jnp.sum(page_sum * factor, axis=0))
        return (numerator / denominator[..., None]).reshape(QUERY_HEADS * HEAD_DIMENSION)
    attention = lax.map(per_request, (queries, lengths, page_table))
    return jnp.dot(attention.astype(jnp.bfloat16), out_weight, preferred_element_type=jnp.float32).astype(jnp.bfloat16)
```

```python
import functools
import math

import jax
import jax.numpy as jnp
from jax import lax
from jax.experimental import pallas as pl
from jax.experimental.pallas import tpu as pltpu
from jax.sharding import PartitionSpec as P

floor_score = -1e30
DIGIT = 32
GROUP = 8
LANES = 128


def locate_kernel(page_size, table_ref, lengths_ref, out_ref, acc):
    requests, width = table_ref.shape
    rows = out_ref.shape[0]
    step = 8
    acc[...] = jnp.zeros_like(acc)
    iota_hi = lax.broadcasted_iota(jnp.int32, (rows, width), 0)
    iota_lo = lax.broadcasted_iota(jnp.int32, (DIGIT, width), 0)
    entry = lax.broadcasted_iota(jnp.int32, (1, width), 1) * page_size

    def body(i, carry):
        lefts, rights = [], []
        block = table_ref[pl.ds(pl.multiple_of(i * step, step), step), :]
        for s in range(step):
            r = i * step + s
            row = block[s : s + 1, :]
            hi = row >> 5
            lo = row & (DIGIT - 1)
            live = jnp.minimum(lengths_ref[r] - entry, page_size).astype(jnp.float32)
            lefts.append(jnp.where(iota_hi == hi, 1.0, 0.0).astype(jnp.bfloat16))
            same = iota_lo == lo
            r_high = (r // 256).astype(jnp.float32)
            r_low = (r % 256).astype(jnp.float32)
            parts = [
                jnp.where(same, r_high, 0.0),
                jnp.where(same, r_low, 0.0),
                jnp.where(same, live, 0.0),
            ]
            rights.append(jnp.concatenate(parts, axis=0).astype(jnp.bfloat16))
        left = jnp.concatenate(lefts, axis=1)
        right = jnp.concatenate(rights, axis=1)
        acc[...] += lax.dot_general(
            left, right, (((1,), (1,)), ((), ())), preferred_element_type=jnp.float32
        )
        return carry

    lax.fori_loop(0, requests // step, body, 0)
    out_ref[...] = acc[...]


def attend_kernel(
    kv_local,
    q_ref,
    member_ref,
    scale_ref,
    bias_ref,
    block_ref,
    vscale_ref,
    k_ref,
    v_ref,
    out_ref,
    q_rows,
    m_rows,
    sums,
    shift,
    extra,
):
    heads, pages, dim = q_rows.shape
    requests = q_ref.shape[0]
    group_rows = block_ref.shape[1]
    per_head = heads // kv_local
    steps = pl.num_programs(0)
    pid = pl.program_id(0)
    groups = k_ref.shape[0] // group_rows

    @pl.when(pid == 0)
    def _():
        member = member_ref[...].astype(jnp.bfloat16)

        def pick(i, carry):
            cols = q_ref[:, pl.ds(pl.multiple_of(i * 2 * dim, 2 * dim), 2 * dim)]
            got = jnp.dot(member, cols, preferred_element_type=jnp.float32)
            q_rows[2 * i] = got[:, :dim]
            q_rows[2 * i + 1] = got[:, dim:]
            return carry

        lax.fori_loop(0, heads // 2, pick, 0)

    def group(i, carry):
        g = pid * groups + i
        p0 = pl.multiple_of(g * GROUP, GROUP)
        q = jnp.concatenate([q_rows[h, pl.ds(p0, GROUP), :] for h in range(heads)], axis=0)
        start = pl.multiple_of(i * group_rows, group_rows)
        kk = k_ref[pl.ds(start, group_rows), :]
        vv = v_ref[pl.ds(start, group_rows), :]
        s = lax.dot_general(
            q.astype(jnp.bfloat16), kk, (((1,), (1,)), ((), ())), preferred_element_type=jnp.float32
        )
        s = (s * scale_ref[pl.ds(g, 1), :] + bias_ref[pl.ds(g, 1), :]) + block_ref[...]
        top = jnp.max(s, axis=1, keepdims=True)
        w = jnp.exp(s - top).astype(jnp.bfloat16)
        both = jnp.concatenate([vv, jnp.ones_like(vv)], axis=1)
        o = jnp.dot(w, both, preferred_element_type=jnp.float32)
        factors = [vscale_ref[pl.ds(p0, GROUP), k : k + 1] for k in range(kv_local)]
        for h in range(heads):
            rows = slice(h * GROUP, (h + 1) * GROUP)
            sums[h, pl.ds(p0, GROUP), :dim] = o[rows, :dim] * factors[h // per_head]
            sums[h, pl.ds(p0, GROUP), dim:] = o[rows, dim:]
            m_rows[h, pl.ds(p0, GROUP), :] = jnp.broadcast_to(top[rows], (GROUP, dim))
        return carry

    lax.fori_loop(0, groups, group, 0, unroll=4)

    @pl.when(pid == steps - 1)
    def _():
        shift[...] = jnp.zeros_like(shift)
        extra[...] = jnp.zeros_like(extra)
        lane = lax.broadcasted_iota(jnp.int32, extra.shape, 1)

        def finish(h, carry):
            inside = member_ref[...] > 0.5
            top = jnp.concatenate([m_rows[h]] * (requests // dim), axis=1)
            peak = jnp.max(jnp.where(inside, top, floor_score), axis=0, keepdims=True)
            peak = peak.astype(jnp.bfloat16).astype(jnp.float32)
            f = jnp.where(inside, jnp.exp(top - peak), 0.0).astype(jnp.bfloat16)
            got = lax.dot_general(
                f,
                sums[h].astype(jnp.bfloat16),
                (((0,), (0,)), ((), ())),
                preferred_element_type=jnp.float32,
            )
            cols = pl.ds(pl.multiple_of(h * dim, dim), dim)
            out_ref[:, cols] = got[:, :dim].astype(jnp.bfloat16)
            den = got[:, dim:]
            den_high = den.astype(jnp.bfloat16).astype(jnp.float32)
            kept = jnp.where(lane == h, den_high, extra[...])
            extra[...] = jnp.where(lane == heads + h, den - den_high, kept)
            shift[pl.ds(2 * heads + h, 1), :] = peak
            return carry

        lax.fori_loop(0, heads, finish, 0)
        tail = jnp.where(lane < 2 * heads, extra[...], shift[...].T)
        out_ref[:, heads * dim :] = tail.astype(jnp.bfloat16)


def on_device(
    queries,
    k_codes,
    value_quantized_codes,
    key_page_scale,
    value_page_scale,
    lengths,
    page_table,
    out_weight,
):
    pages, page_size, kv_local, dim = k_codes.shape
    rows_here, heads, _ = queries.shape
    per_head = heads // kv_local
    width = heads * dim
    vmem = pl.BlockSpec(memory_space=pltpu.VMEM)
    smem = pl.BlockSpec(memory_space=pltpu.SMEM)

    table = lax.all_gather(page_table, "req", axis=0, tiled=True)
    all_lengths = lax.all_gather(lengths, "req", axis=0, tiled=True)
    q_all = lax.all_gather(queries.reshape(rows_here, width), "req", axis=0, tiled=True)
    requests = table.shape[0]
    sources = lax.axis_size("req")
    local_table = table - lax.axis_index("req") * pages

    found = pl.pallas_call(
        functools.partial(locate_kernel, page_size),
        out_shape=jax.ShapeDtypeStruct((pages // DIGIT, 3 * DIGIT), jnp.float32),
        in_specs=[vmem, smem],
        out_specs=vmem,
        scratch_shapes=[pltpu.VMEM((pages // DIGIT, 3 * DIGIT), jnp.float32)],
        name="locate",
    )(local_table, all_lengths)
    owner = (found[:, :DIGIT] * 256.0 + found[:, DIGIT : 2 * DIGIT]).reshape(pages)
    live = found[:, 2 * DIGIT :].reshape(pages)
    ids = jnp.arange(requests, dtype=jnp.int32).astype(jnp.float32)
    member = (owner[:, None] == ids[None, :]).astype(jnp.float32)

    page_rows = page_size * kv_local
    group_rows = GROUP * page_rows
    token = jnp.arange(page_size, dtype=jnp.int32).astype(jnp.float32)[None, :, None]
    full = (pages, page_size, kv_local)
    bias = jnp.where(jnp.broadcast_to(token < live[:, None, None], full), 0.0, floor_score)
    bias = bias.reshape(pages // GROUP, group_rows)
    scale = jnp.broadcast_to(key_page_scale[:, None, :] / math.sqrt(dim), full)
    scale = scale.reshape(pages // GROUP, group_rows)
    row = jnp.arange(heads * GROUP, dtype=jnp.int32)[:, None]
    col = jnp.arange(group_rows, dtype=jnp.int32)[None, :]
    same = (row % GROUP == col // page_rows) & (row // GROUP // per_head == col % kv_local)
    block = jnp.where(same, 0.0, floor_score).astype(jnp.float32)

    k_rows = k_codes.reshape(pages * page_rows, dim)
    v_rows = value_quantized_codes.reshape(pages * page_rows, dim)
    block_pages = 128
    steps = pages // block_pages
    whole = lambda shape: pl.BlockSpec(shape, lambda i: (0,) * len(shape))
    stream = pl.BlockSpec((block_pages * page_rows, dim), lambda i: (i, 0))
    partial_sums = pl.pallas_call(
        functools.partial(attend_kernel, kv_local),
        grid=(steps,),
        out_shape=jax.ShapeDtypeStruct((requests, width + LANES), jnp.bfloat16),
        in_specs=[vmem, vmem, vmem, vmem, vmem, vmem, stream, stream],
        out_specs=whole((requests, width + LANES)),
        scratch_shapes=[
            pltpu.VMEM((heads, pages, dim), jnp.float32),
            pltpu.VMEM((heads, pages, dim), jnp.float32),
            pltpu.VMEM((heads, pages, 2 * dim), jnp.float32),
            pltpu.VMEM((LANES, requests), jnp.float32),
            pltpu.VMEM((requests, LANES), jnp.float32),
        ],
        compiler_params=pltpu.CompilerParams(
            vmem_limit_bytes=60 * 1024 * 1024, dimension_semantics=("arbitrary",)
        ),
        name="attend",
    )(q_all, member, scale, bias, block, value_page_scale, k_rows, v_rows)

    got = lax.all_to_all(
        partial_sums.reshape(sources, rows_here, width + LANES),
        "req",
        split_axis=0,
        concat_axis=0,
        tiled=True,
    ).astype(jnp.float32)
    tail = got[:, :, width:]
    den = tail[:, :, :heads] + tail[:, :, heads : 2 * heads]
    peak = tail[:, :, 2 * heads : 3 * heads]
    factor = jnp.exp(peak - jnp.max(peak, axis=0)[None])
    factor = factor / jnp.sum(den * factor, axis=0)[None]
    numer = got[:, :, :width].reshape(sources, rows_here, heads, dim)
    attention = jnp.sum(numer * factor[..., None], axis=0).reshape(rows_here, width)
    terms = jnp.dot(
        lax.all_gather(attention.astype(jnp.bfloat16), "req", axis=0, tiled=True),
        out_weight,
        preferred_element_type=jnp.float32,
    )
    return lax.psum_scatter(terms.astype(jnp.bfloat16), "head", scatter_dimension=1, tiled=True)


def solution(mesh):
    in_specs = (
        P("req", "head", None),
        P("req", None, "head", None),
        P("req", None, "head", None),
        P("req", "head"),
        P("req", "head"),
        P("req"),
        P("req", None),
        P("head", "req"),
    )
    out_specs = P(None, ("req", "head"))
    return jax.shard_map(
        on_device, mesh=mesh, in_specs=in_specs, out_specs=out_specs, check_vma=False
    )
```

```python
import functools
import math

import jax
import jax.numpy as jnp
from jax import lax
from jax.experimental import pallas as pl
from jax.experimental.pallas import tpu as pltpu
from jax.sharding import PartitionSpec as P

floor_score = -1e30
GROUP = 8
LANES = 128


def greet(peers):
    barrier = pltpu.get_barrier_semaphore()
    for peer in peers:
        pl.semaphore_signal(
            barrier, inc=1, device_id=peer, device_id_type=pl.DeviceIdType.MESH
        )
    pl.semaphore_wait(barrier, len(peers))


def send(src, dst, send_sem, recv_sem, peer):
    copy = pltpu.make_async_remote_copy(
        src_ref=src,
        dst_ref=dst,
        send_sem=send_sem,
        recv_sem=recv_sem,
        device_id=peer,
        device_id_type=pl.DeviceIdType.MESH,
    )
    copy.start()
    return copy


def gather_kernel(
    sources, base, code_ref, q_ref, found_ref, q_all, codes, acc, q_send, q_recv, c_send, c_recv
):
    me, z = lax.axis_index("req"), lax.axis_index("head")
    rows, width = code_ref.shape
    requests = codes.shape[0]
    high_rows = found_ref.shape[0]
    peers = [(lax.rem(me + d, sources), z) for d in range(1, sources)]
    greet(peers)
    mine = pl.ds(pl.multiple_of(me * rows, rows), rows)
    code_copies = [
        send(code_ref, codes.at[mine], c_send.at[i], c_recv.at[i], peer)
        for i, peer in enumerate(peers)
    ]
    q_copies = [
        send(q_ref, q_all.at[mine], q_send.at[i], q_recv.at[i], peer)
        for i, peer in enumerate(peers)
    ]
    codes[mine, :] = code_ref[...]
    q_all[mine, :] = q_ref[...]
    for copy in code_copies:
        copy.wait()

    acc[...] = jnp.zeros_like(acc)
    iota_hi = lax.broadcasted_iota(jnp.int32, (high_rows, width), 0)
    iota_lo = lax.broadcasted_iota(jnp.int32, (GROUP, width), 0)
    offset = me * (high_rows * GROUP)
    step = 8

    def body(i, carry):
        lefts, rights = [], []
        block = codes[pl.ds(pl.multiple_of(i * step, step), step), :]
        page = (block >> base) - offset
        live_all = (block & ((1 << base) - 1)).astype(jnp.float32)
        for t in range(step):
            r = i * step + t
            row = page[t : t + 1, :]
            lefts.append(jnp.where(iota_hi == (row >> 3), 1.0, 0.0).astype(jnp.bfloat16))
            same = iota_lo == (row & (GROUP - 1))
            parts = [
                jnp.where(same, (r // 256).astype(jnp.float32), 0.0),
                jnp.where(same, (r % 256).astype(jnp.float32), 0.0),
                jnp.where(same, live_all[t : t + 1, :], 0.0),
                jnp.zeros(same.shape, jnp.float32),
            ]
            rights.append(jnp.concatenate(parts, axis=0).astype(jnp.bfloat16))
        acc[...] += lax.dot_general(
            jnp.concatenate(lefts, axis=1),
            jnp.concatenate(rights, axis=1),
            (((1,), (1,)), ((), ())),
            preferred_element_type=jnp.float32,
        )
        return carry

    lax.fori_loop(0, requests // step, body, 0)
    found_ref[...] = acc[...]
    for copy in q_copies:
        copy.wait()


def project_kernel(
    sources,
    parts,
    heads,
    sums_ref,
    weight_ref,
    out_ref,
    weight,
    got,
    own,
    rows_all,
    terms,
    terms_in,
    w_sem,
    s_send,
    s_recv,
    a_send,
    a_recv,
    t_send,
    t_recv,
):
    me, z = lax.axis_index("req"), lax.axis_index("head")
    rows = own.shape[0]
    dim = LANES
    load = pltpu.make_async_copy(weight_ref, weight, w_sem)
    load.start()
    peers = [(lax.rem(me + d, sources), z) for d in range(1, sources)]
    others = [(me, lax.rem(z + d, parts)) for d in range(1, parts)]
    greet(peers + others)
    copies = []
    for i, peer in enumerate(peers):
        theirs = pl.ds(pl.multiple_of(peer[0] * rows, rows), rows)
        copies.append(send(sums_ref.at[theirs], got.at[me], s_send.at[i], s_recv.at[i], peer))
    mine = pl.ds(pl.multiple_of(me * rows, rows), rows)
    got[me] = sums_ref[mine, :]
    for copy in copies:
        copy.wait()

    tails = [got[i, :, heads * dim :].astype(jnp.float32) for i in range(sources)]
    peaks = [t[:, 2 * heads : 3 * heads] for t in tails]
    top = functools.reduce(jnp.maximum, peaks)
    factors = [jnp.exp(p - top) for p in peaks]
    dens = [t[:, :heads] + t[:, heads : 2 * heads] for t in tails]
    total = functools.reduce(jnp.add, [f * d for f, d in zip(factors, dens)])
    factors = [f / total for f in factors]
    for h in range(heads):
        cols = slice(h * dim, (h + 1) * dim)
        value = jnp.zeros((rows, dim), jnp.float32)
        for i in range(sources):
            value += got[i, :, cols].astype(jnp.float32) * factors[i][:, h : h + 1]
        own[:, cols] = value.astype(jnp.bfloat16)
    copies = [
        send(own, rows_all.at[mine], a_send.at[i], a_recv.at[i], peer)
        for i, peer in enumerate(peers)
    ]
    rows_all[mine, :] = own[...]
    load.wait()
    for copy in copies:
        copy.wait()

    width = out_ref.shape[1]

    def product(part):
        cols = pl.ds(pl.multiple_of(part * width, width), width)
        return jnp.dot(rows_all[...], weight[:, cols], preferred_element_type=jnp.float32)

    aligned = width % LANES == 0
    if not aligned:
        full = jnp.dot(rows_all[...], weight[...], preferred_element_type=jnp.float32)
        for part in range(parts):
            terms[part] = full[:, part * width : (part + 1) * width].astype(jnp.bfloat16)
    copies = []
    for i, peer in enumerate(others):
        part = peer[1]
        if aligned:
            terms[part] = product(part).astype(jnp.bfloat16)
        copies.append(send(terms.at[part], terms_in.at[i], t_send.at[i], t_recv.at[i], peer))
    result = product(z) if aligned else terms[z].astype(jnp.float32)
    for i, copy in enumerate(copies):
        copy.wait()
        result += terms_in[i].astype(jnp.float32)
    out_ref[...] = result.astype(jnp.bfloat16)


def attend_kernel(
    kv_local,
    page_size,
    q_ref,
    found_ref,
    kscale_ref,
    vscale_ref,
    k_ref,
    v_ref,
    out_ref,
    member_ref,
    bias_ref,
    block_ref,
    scales,
    q_rows,
    m_rows,
    sums,
    shift,
    extra,
):
    heads, pages, dim = q_rows.shape
    requests = q_ref.shape[0]
    group_rows = bias_ref.shape[1]
    per_head = heads // kv_local
    steps = pl.num_programs(0)
    pid = pl.program_id(0)
    groups = k_ref.shape[0] // group_rows

    @pl.when(pid == 0)
    def _():
        found = found_ref[...].astype(jnp.bfloat16)
        page_rows = page_size * kv_local
        iota = lambda shape, axis: lax.broadcasted_iota(jnp.int32, shape, axis)
        spread_shape = (found.shape[1], group_rows)
        spread = iota(spread_shape, 0) - 2 * GROUP == iota(spread_shape, 1) // page_rows
        spread = jnp.where(spread, 1.0, 0.0).astype(jnp.bfloat16)
        live = jnp.dot(found, spread, preferred_element_type=jnp.float32)
        token = (iota(live.shape, 1) % page_rows) // kv_local
        bias_ref[...] = jnp.where(token.astype(jnp.float32) < live, 0.0, floor_score)
        row, col = iota(block_ref.shape, 0), iota(block_ref.shape, 1)
        same = (row % GROUP == col // page_rows) & (row // GROUP // per_head == col % kv_local)
        block_ref[...] = jnp.where(same, 0.0, floor_score)
        repeat_shape = (pages, found.shape[0])
        repeat = iota(repeat_shape, 0) // GROUP == iota(repeat_shape, 1)
        repeat = jnp.where(repeat, 1.0, 0.0).astype(jnp.bfloat16)
        rows = jnp.dot(repeat, found, preferred_element_type=jnp.float32)
        lane, slot = iota(rows.shape, 1), iota(rows.shape, 0) % GROUP
        digit = jnp.where(lane == slot, 256.0, jnp.where(lane == slot + GROUP, 1.0, 0.0))
        owner = jnp.sum(rows * digit, axis=1, keepdims=True)
        ids = iota(member_ref.shape, 1).astype(jnp.float32)
        member_ref[...] = jnp.where(owner == ids, 1.0, 0.0)
        member = member_ref[...].astype(jnp.bfloat16)
        root = 1.0 / math.sqrt(dim)
        spare = jnp.zeros((8 - 2 * kv_local, pages), jnp.float32)
        stacked = jnp.concatenate([kscale_ref[...] * root, vscale_ref[...], spare], axis=0)
        scales[...] = stacked.T

        def pick(i, carry):
            cols = q_ref[:, pl.ds(pl.multiple_of(i * 2 * dim, 2 * dim), 2 * dim)]
            got = jnp.dot(member, cols, preferred_element_type=jnp.float32)
            q_rows[2 * i] = got[:, :dim]
            q_rows[2 * i + 1] = got[:, dim:]
            return carry

        lax.fori_loop(0, heads // 2, pick, 0)

    def group(i, carry):
        g = pid * groups + i
        p0 = pl.multiple_of(g * GROUP, GROUP)
        q = jnp.concatenate([q_rows[h, pl.ds(p0, GROUP), :] for h in range(heads)], axis=0)
        start = pl.multiple_of(i * group_rows, group_rows)
        kk = k_ref[pl.ds(start, group_rows), :]
        vv = v_ref[pl.ds(start, group_rows), :]
        s = lax.dot_general(
            q.astype(jnp.bfloat16), kk, (((1,), (1,)), ((), ())), preferred_element_type=jnp.float32
        )
        factors = [scales[pl.ds(p0, GROUP), k : k + 1] for k in range(2 * kv_local)]
        row_scale = jnp.concatenate([factors[h // per_head] for h in range(heads)], axis=0)
        s = (s * row_scale + bias_ref[pl.ds(g, 1), :]) + block_ref[...]
        top = jnp.max(s, axis=1, keepdims=True)
        w = jnp.exp(s - top).astype(jnp.bfloat16)
        both = jnp.concatenate([vv, jnp.ones_like(vv)], axis=1)
        o = jnp.dot(w, both, preferred_element_type=jnp.float32)
        for h in range(heads):
            rows = slice(h * GROUP, (h + 1) * GROUP)
            sums[h, pl.ds(p0, GROUP), :dim] = o[rows, :dim] * factors[kv_local + h // per_head]
            sums[h, pl.ds(p0, GROUP), dim:] = o[rows, dim:]
            m_rows[h, pl.ds(p0, GROUP), :] = jnp.broadcast_to(top[rows], (GROUP, dim))
        return carry

    lax.fori_loop(0, groups, group, 0, unroll=4)

    @pl.when(pid == steps - 1)
    def _():
        shift[...] = jnp.zeros_like(shift)
        extra[...] = jnp.zeros_like(extra)
        lane = lax.broadcasted_iota(jnp.int32, extra.shape, 1)

        def finish(h, carry):
            inside = member_ref[...] > 0.5
            top = jnp.concatenate([m_rows[h]] * (requests // dim), axis=1)
            peak = jnp.max(jnp.where(inside, top, floor_score), axis=0, keepdims=True)
            peak = peak.astype(jnp.bfloat16).astype(jnp.float32)
            f = jnp.where(inside, jnp.exp(top - peak), 0.0).astype(jnp.bfloat16)
            got = lax.dot_general(
                f,
                sums[h].astype(jnp.bfloat16),
                (((0,), (0,)), ((), ())),
                preferred_element_type=jnp.float32,
            )
            cols = pl.ds(pl.multiple_of(h * dim, dim), dim)
            out_ref[:, cols] = got[:, :dim].astype(jnp.bfloat16)
            den = got[:, dim:]
            den_high = den.astype(jnp.bfloat16).astype(jnp.float32)
            kept = jnp.where(lane == h, den_high, extra[...])
            extra[...] = jnp.where(lane == heads + h, den - den_high, kept)
            shift[pl.ds(2 * heads + h, 1), :] = peak
            return carry

        lax.fori_loop(0, heads, finish, 0)
        tail = jnp.where(lane < 2 * heads, extra[...], shift[...].T)
        out_ref[:, heads * dim :] = tail.astype(jnp.bfloat16)


def on_device(
    queries,
    k_codes,
    value_quantized_codes,
    key_page_scale,
    value_page_scale,
    lengths,
    page_table,
    out_weight,
):
    pages, page_size, kv_local, dim = k_codes.shape
    rows_here, heads, _ = queries.shape
    width = heads * dim
    vmem = pl.BlockSpec(memory_space=pltpu.VMEM)
    sources, parts = lax.axis_size("req"), lax.axis_size("head")
    requests = sources * rows_here
    table_width = page_table.shape[1]
    base = page_size.bit_length()
    entry = jnp.arange(table_width, dtype=jnp.int32)[None, :] * page_size
    live = jnp.clip(lengths[:, None] - entry, 0, page_size)
    code = jnp.where(live > 0, page_table * (1 << base) + live, -1)

    dma = pltpu.SemaphoreType.DMA
    groups = pages // GROUP
    found, q_all = pl.pallas_call(
        functools.partial(gather_kernel, sources, base),
        out_shape=[
            jax.ShapeDtypeStruct((groups, 4 * GROUP), jnp.float32),
            jax.ShapeDtypeStruct((requests, width), jnp.bfloat16),
        ],
        in_specs=[vmem, vmem],
        out_specs=[vmem, vmem],
        scratch_shapes=[
            pltpu.VMEM((requests, table_width), jnp.int32),
            pltpu.VMEM((groups, 4 * GROUP), jnp.float32),
        ]
        + [dma((sources - 1,))] * 4,
        compiler_params=pltpu.CompilerParams(collective_id=0, has_side_effects=True),
        name="gather",
    )(code, queries.reshape(rows_here, width))

    page_rows = page_size * kv_local
    group_rows = GROUP * page_rows
    k_rows = k_codes.reshape(pages * page_rows, dim)
    v_rows = value_quantized_codes.reshape(pages * page_rows, dim)
    block_pages = 128
    steps = pages // block_pages
    whole = lambda shape: pl.BlockSpec(shape, lambda i: (0,) * len(shape))
    stream = pl.BlockSpec((block_pages * page_rows, dim), lambda i: (i, 0))
    partial_sums = pl.pallas_call(
        functools.partial(attend_kernel, kv_local, page_size),
        grid=(steps,),
        out_shape=jax.ShapeDtypeStruct((requests, width + LANES), jnp.bfloat16),
        in_specs=[vmem, vmem, vmem, vmem, stream, stream],
        out_specs=whole((requests, width + LANES)),
        scratch_shapes=[
            pltpu.VMEM((pages, requests), jnp.float32),
            pltpu.VMEM((groups, group_rows), jnp.float32),
            pltpu.VMEM((heads * GROUP, group_rows), jnp.float32),
            pltpu.VMEM((pages, 8), jnp.float32),
            pltpu.VMEM((heads, pages, dim), jnp.float32),
            pltpu.VMEM((heads, pages, dim), jnp.float32),
            pltpu.VMEM((heads, pages, 2 * dim), jnp.float32),
            pltpu.VMEM((LANES, requests), jnp.float32),
            pltpu.VMEM((requests, LANES), jnp.float32),
        ],
        compiler_params=pltpu.CompilerParams(
            vmem_limit_bytes=60 * 1024 * 1024, dimension_semantics=("arbitrary",)
        ),
        name="attend",
    )(q_all, found, key_page_scale.T, value_page_scale.T, k_rows, v_rows)

    columns = out_weight.shape[1] // parts
    return pl.pallas_call(
        functools.partial(project_kernel, sources, parts, heads),
        out_shape=jax.ShapeDtypeStruct((requests, columns), jnp.bfloat16),
        in_specs=[vmem, pl.BlockSpec(memory_space=pl.ANY)],
        out_specs=vmem,
        scratch_shapes=[
            pltpu.VMEM(out_weight.shape, jnp.bfloat16),
            pltpu.VMEM((sources, rows_here, width + LANES), jnp.bfloat16),
            pltpu.VMEM((rows_here, width), jnp.bfloat16),
            pltpu.VMEM((requests, width), jnp.bfloat16),
            pltpu.VMEM((parts, requests, columns), jnp.bfloat16),
            pltpu.VMEM((parts - 1, requests, columns), jnp.bfloat16),
            dma,
        ]
        + [dma((sources - 1,))] * 4
        + [dma((parts - 1,))] * 2,
        compiler_params=pltpu.CompilerParams(
            collective_id=1, has_side_effects=True, vmem_limit_bytes=40 * 1024 * 1024
        ),
        name="project",
    )(partial_sums, out_weight)


def solution(mesh):
    in_specs = (
        P("req", "head", None),
        P("req", None, "head", None),
        P("req", None, "head", None),
        P("req", "head"),
        P("req", "head"),
        P("req"),
        P("req", None),
        P("head", "req"),
    )
    out_specs = P(None, ("req", "head"))
    return jax.shard_map(
        on_device, mesh=mesh, in_specs=in_specs, out_specs=out_specs, check_vma=False
    )
```

```python
import functools
import math

import jax
import jax.numpy as jnp
from jax import lax
from jax.experimental import pallas as pl
from jax.experimental.pallas import tpu as pltpu
from jax.sharding import PartitionSpec as P

floor_score = -1e30
GROUP = 8
LANES = 128


def greet(peers):
    barrier = pltpu.get_barrier_semaphore()
    for peer in peers:
        pl.semaphore_signal(
            barrier, inc=1, device_id=peer, device_id_type=pl.DeviceIdType.MESH
        )
    pl.semaphore_wait(barrier, len(peers))


def send(src, dst, send_sem, recv_sem, peer):
    copy = pltpu.make_async_remote_copy(
        src_ref=src,
        dst_ref=dst,
        send_sem=send_sem,
        recv_sem=recv_sem,
        device_id=peer,
        device_id_type=pl.DeviceIdType.MESH,
    )
    copy.start()
    return copy


def gather_kernel(
    sources, base, code_ref, q_ref, found_ref, q_all, codes, acc, q_send, q_recv, c_send, c_recv
):
    me, z = lax.axis_index("req"), lax.axis_index("head")
    rows, width = code_ref.shape
    requests = codes.shape[0]
    high_rows = found_ref.shape[0]
    peers = [(lax.rem(me + d, sources), z) for d in range(1, sources)]
    greet(peers)
    mine = pl.ds(pl.multiple_of(me * rows, rows), rows)
    code_copies = [
        send(code_ref, codes.at[mine], c_send.at[i], c_recv.at[i], peer)
        for i, peer in enumerate(peers)
    ]
    q_copies = [
        send(q_ref, q_all.at[mine], q_send.at[i], q_recv.at[i], peer)
        for i, peer in enumerate(peers)
    ]
    codes[mine, :] = code_ref[...]
    q_all[mine, :] = q_ref[...]
    for copy in code_copies:
        copy.wait()

    acc[...] = jnp.zeros_like(acc)
    iota_hi = lax.broadcasted_iota(jnp.int32, (high_rows, width), 0)
    iota_lo = lax.broadcasted_iota(jnp.int32, (GROUP, width), 0)
    offset = me * (high_rows * GROUP)
    step = 8

    def body(i, carry):
        lefts, rights = [], []
        block = codes[pl.ds(pl.multiple_of(i * step, step), step), :]
        page = (block >> base) - offset
        live_all = (block & ((1 << base) - 1)).astype(jnp.float32)
        for t in range(step):
            r = i * step + t
            row = page[t : t + 1, :]
            lefts.append(jnp.where(iota_hi == (row >> 3), 1.0, 0.0).astype(jnp.bfloat16))
            same = iota_lo == (row & (GROUP - 1))
            parts = [
                jnp.where(same, (r // 256).astype(jnp.float32), 0.0),
                jnp.where(same, (r % 256).astype(jnp.float32), 0.0),
                jnp.where(same, live_all[t : t + 1, :], 0.0),
                jnp.zeros(same.shape, jnp.float32),
            ]
            rights.append(jnp.concatenate(parts, axis=0).astype(jnp.bfloat16))
        acc[...] += lax.dot_general(
            jnp.concatenate(lefts, axis=1),
            jnp.concatenate(rights, axis=1),
            (((1,), (1,)), ((), ())),
            preferred_element_type=jnp.float32,
        )
        return carry

    lax.fori_loop(0, requests // step, body, 0, unroll=2)
    found_ref[...] = acc[...]
    for copy in q_copies:
        copy.wait()


def project_kernel(
    sources,
    parts,
    heads,
    sums_ref,
    weight_ref,
    out_ref,
    weight,
    got,
    own,
    rows_all,
    terms,
    terms_in,
    w_sem,
    s_send,
    s_recv,
    a_send,
    a_recv,
    t_send,
    t_recv,
):
    me, z = lax.axis_index("req"), lax.axis_index("head")
    rows = own.shape[0]
    dim = LANES
    load = pltpu.make_async_copy(weight_ref, weight, w_sem)
    load.start()
    peers = [(lax.rem(me + d, sources), z) for d in range(1, sources)]
    others = [(me, lax.rem(z + d, parts)) for d in range(1, parts)]
    greet(peers + others)
    copies = []
    for i, peer in enumerate(peers):
        theirs = pl.ds(pl.multiple_of(peer[0] * rows, rows), rows)
        copies.append(send(sums_ref.at[theirs], got.at[me], s_send.at[i], s_recv.at[i], peer))
    mine = pl.ds(pl.multiple_of(me * rows, rows), rows)
    got[me] = sums_ref[mine, :]
    for copy in copies:
        copy.wait()

    tails = [got[i, :, heads * dim :].astype(jnp.float32) for i in range(sources)]
    peaks = [t[:, 2 * heads : 3 * heads] for t in tails]
    top = functools.reduce(jnp.maximum, peaks)
    factors = [jnp.exp(p - top) for p in peaks]
    dens = [t[:, :heads] + t[:, heads : 2 * heads] for t in tails]
    total = functools.reduce(jnp.add, [f * d for f, d in zip(factors, dens)])
    factors = [f / total for f in factors]
    for h in range(heads):
        cols = slice(h * dim, (h + 1) * dim)
        value = jnp.zeros((rows, dim), jnp.float32)
        for i in range(sources):
            value += got[i, :, cols].astype(jnp.float32) * factors[i][:, h : h + 1]
        own[:, cols] = value.astype(jnp.bfloat16)
    copies = [
        send(own, rows_all.at[mine], a_send.at[i], a_recv.at[i], peer)
        for i, peer in enumerate(peers)
    ]
    rows_all[mine, :] = own[...]
    load.wait()
    for copy in copies:
        copy.wait()

    width = out_ref.shape[1]

    def product(part):
        cols = pl.ds(pl.multiple_of(part * width, width), width)
        return jnp.dot(rows_all[...], weight[:, cols], preferred_element_type=jnp.float32)

    aligned = width % LANES == 0
    if not aligned:
        full = jnp.dot(rows_all[...], weight[...], preferred_element_type=jnp.float32)
        for part in range(parts):
            terms[part] = full[:, part * width : (part + 1) * width].astype(jnp.bfloat16)
    copies = []
    for i, peer in enumerate(others):
        part = peer[1]
        if aligned:
            terms[part] = product(part).astype(jnp.bfloat16)
        copies.append(send(terms.at[part], terms_in.at[i], t_send.at[i], t_recv.at[i], peer))
    result = product(z) if aligned else terms[z].astype(jnp.float32)
    for i, copy in enumerate(copies):
        copy.wait()
        result += terms_in[i].astype(jnp.float32)
    out_ref[...] = result.astype(jnp.bfloat16)


def attend_kernel(
    kv_local,
    page_size,
    q_ref,
    found_ref,
    kscale_ref,
    vscale_ref,
    k_ref,
    v_ref,
    out_ref,
    member_ref,
    bias_ref,
    block_ref,
    scales,
    q_rows,
    m_rows,
    sums,
    shift,
    extra,
):
    heads, pages, dim = q_rows.shape
    requests = q_ref.shape[0]
    group_rows = bias_ref.shape[1]
    per_head = heads // kv_local
    steps = pl.num_programs(0)
    pid = pl.program_id(0)
    groups = k_ref.shape[0] // group_rows

    @pl.when(pid == 0)
    def _():
        found = found_ref[...].astype(jnp.bfloat16)
        page_rows = page_size * kv_local
        iota = lambda shape, axis: lax.broadcasted_iota(jnp.int32, shape, axis)
        spread_shape = (found.shape[1], group_rows)
        spread = iota(spread_shape, 0) - 2 * GROUP == iota(spread_shape, 1) // page_rows
        spread = jnp.where(spread, 1.0, 0.0).astype(jnp.bfloat16)
        live = jnp.dot(found, spread, preferred_element_type=jnp.float32)
        token = (iota(live.shape, 1) % page_rows) // kv_local
        bias_ref[...] = jnp.where(token.astype(jnp.float32) < live, 0.0, floor_score)
        row, col = iota(block_ref.shape, 0), iota(block_ref.shape, 1)
        same = (row % GROUP == col // page_rows) & (row // GROUP // per_head == col % kv_local)
        block_ref[...] = jnp.where(same, 0.0, floor_score)
        repeat_shape = (pages, found.shape[0])
        repeat = iota(repeat_shape, 0) // GROUP == iota(repeat_shape, 1)
        repeat = jnp.where(repeat, 1.0, 0.0).astype(jnp.bfloat16)
        rows = jnp.dot(repeat, found, preferred_element_type=jnp.float32)
        lane, slot = iota(rows.shape, 1), iota(rows.shape, 0) % GROUP
        digit = jnp.where(lane == slot, 256.0, jnp.where(lane == slot + GROUP, 1.0, 0.0))
        owner = jnp.sum(rows * digit, axis=1, keepdims=True)
        ids = iota(member_ref.shape, 1).astype(jnp.float32)
        member_ref[...] = jnp.where(owner == ids, 1.0, 0.0)
        member = member_ref[...].astype(jnp.bfloat16)
        root = 1.0 / math.sqrt(dim)
        spare = jnp.zeros((8 - 2 * kv_local, pages), jnp.float32)
        stacked = jnp.concatenate([kscale_ref[...] * root, vscale_ref[...], spare], axis=0)
        scales[...] = stacked.T

        def pick(i, carry):
            cols = q_ref[:, pl.ds(pl.multiple_of(i * 2 * dim, 2 * dim), 2 * dim)]
            got = jnp.dot(member, cols, preferred_element_type=jnp.float32)
            q_rows[2 * i] = got[:, :dim]
            q_rows[2 * i + 1] = got[:, dim:]
            return carry

        lax.fori_loop(0, heads // 2, pick, 0)

    def group(i, carry):
        g = pid * groups + i
        p0 = pl.multiple_of(g * GROUP, GROUP)
        q = jnp.concatenate([q_rows[h, pl.ds(p0, GROUP), :] for h in range(heads)], axis=0)
        start = pl.multiple_of(i * group_rows, group_rows)
        kk = k_ref[pl.ds(start, group_rows), :]
        vv = v_ref[pl.ds(start, group_rows), :]
        s = lax.dot_general(
            q.astype(jnp.bfloat16), kk, (((1,), (1,)), ((), ())), preferred_element_type=jnp.float32
        )
        factors = [scales[pl.ds(p0, GROUP), k : k + 1] for k in range(2 * kv_local)]
        row_scale = jnp.concatenate([factors[h // per_head] for h in range(heads)], axis=0)
        s = (s * row_scale + bias_ref[pl.ds(g, 1), :]) + block_ref[...]
        top = jnp.max(s, axis=1, keepdims=True)
        w = jnp.exp(s - top).astype(jnp.bfloat16)
        both = jnp.concatenate([vv, jnp.ones_like(vv)], axis=1)
        o = jnp.dot(w, both, preferred_element_type=jnp.float32)
        for h in range(heads):
            rows = slice(h * GROUP, (h + 1) * GROUP)
            sums[h, pl.ds(p0, GROUP), :dim] = o[rows, :dim] * factors[kv_local + h // per_head]
            sums[h, pl.ds(p0, GROUP), dim:] = o[rows, dim:]
            m_rows[h, pl.ds(p0, GROUP), :] = jnp.broadcast_to(top[rows], (GROUP, dim))
        return carry

    lax.fori_loop(0, groups, group, 0, unroll=8)

    @pl.when(pid == steps - 1)
    def _():
        shift[...] = jnp.zeros_like(shift)
        extra[...] = jnp.zeros_like(extra)
        lane = lax.broadcasted_iota(jnp.int32, extra.shape, 1)

        def finish(h, carry):
            inside = member_ref[...] > 0.5
            top = jnp.concatenate([m_rows[h]] * (requests // dim), axis=1)
            peak = jnp.max(jnp.where(inside, top, floor_score), axis=0, keepdims=True)
            peak = peak.astype(jnp.bfloat16).astype(jnp.float32)
            f = jnp.where(inside, jnp.exp(top - peak), 0.0).astype(jnp.bfloat16)
            got = lax.dot_general(
                f,
                sums[h].astype(jnp.bfloat16),
                (((0,), (0,)), ((), ())),
                preferred_element_type=jnp.float32,
            )
            cols = pl.ds(pl.multiple_of(h * dim, dim), dim)
            out_ref[:, cols] = got[:, :dim].astype(jnp.bfloat16)
            den = got[:, dim:]
            den_high = den.astype(jnp.bfloat16).astype(jnp.float32)
            kept = jnp.where(lane == h, den_high, extra[...])
            extra[...] = jnp.where(lane == heads + h, den - den_high, kept)
            shift[pl.ds(2 * heads + h, 1), :] = peak
            return carry

        lax.fori_loop(0, heads, finish, 0, unroll=4)
        tail = jnp.where(lane < 2 * heads, extra[...], shift[...].T)
        out_ref[:, heads * dim :] = tail.astype(jnp.bfloat16)


def on_device(
    queries,
    k_codes,
    value_quantized_codes,
    key_page_scale,
    value_page_scale,
    lengths,
    page_table,
    out_weight,
):
    pages, page_size, kv_local, dim = k_codes.shape
    rows_here, heads, _ = queries.shape
    width = heads * dim
    vmem = pl.BlockSpec(memory_space=pltpu.VMEM)
    sources, parts = lax.axis_size("req"), lax.axis_size("head")
    requests = sources * rows_here
    table_width = page_table.shape[1]
    base = page_size.bit_length()
    entry = jnp.arange(table_width, dtype=jnp.int32)[None, :] * page_size
    live = jnp.clip(lengths[:, None] - entry, 0, page_size)
    code = jnp.where(live > 0, page_table * (1 << base) + live, -1)

    dma = pltpu.SemaphoreType.DMA
    groups = pages // GROUP
    found, q_all = pl.pallas_call(
        functools.partial(gather_kernel, sources, base),
        out_shape=[
            jax.ShapeDtypeStruct((groups, 4 * GROUP), jnp.float32),
            jax.ShapeDtypeStruct((requests, width), jnp.bfloat16),
        ],
        in_specs=[vmem, vmem],
        out_specs=[vmem, vmem],
        scratch_shapes=[
            pltpu.VMEM((requests, table_width), jnp.int32),
            pltpu.VMEM((groups, 4 * GROUP), jnp.float32),
        ]
        + [dma((sources - 1,))] * 4,
        compiler_params=pltpu.CompilerParams(collective_id=0, has_side_effects=True),
        name="gather",
    )(code, queries.reshape(rows_here, width))

    page_rows = page_size * kv_local
    group_rows = GROUP * page_rows
    k_rows = k_codes.reshape(pages * page_rows, dim)
    v_rows = value_quantized_codes.reshape(pages * page_rows, dim)
    block_pages = 128
    steps = pages // block_pages
    whole = lambda shape: pl.BlockSpec(shape, lambda i: (0,) * len(shape))
    stream = pl.BlockSpec((block_pages * page_rows, dim), lambda i: (i, 0))
    partial_sums = pl.pallas_call(
        functools.partial(attend_kernel, kv_local, page_size),
        grid=(steps,),
        out_shape=jax.ShapeDtypeStruct((requests, width + LANES), jnp.bfloat16),
        in_specs=[vmem, vmem, vmem, vmem, stream, stream],
        out_specs=whole((requests, width + LANES)),
        scratch_shapes=[
            pltpu.VMEM((pages, requests), jnp.float32),
            pltpu.VMEM((groups, group_rows), jnp.float32),
            pltpu.VMEM((heads * GROUP, group_rows), jnp.float32),
            pltpu.VMEM((pages, 8), jnp.float32),
            pltpu.VMEM((heads, pages, dim), jnp.float32),
            pltpu.VMEM((heads, pages, dim), jnp.float32),
            pltpu.VMEM((heads, pages, 2 * dim), jnp.float32),
            pltpu.VMEM((LANES, requests), jnp.float32),
            pltpu.VMEM((requests, LANES), jnp.float32),
        ],
        compiler_params=pltpu.CompilerParams(
            vmem_limit_bytes=60 * 1024 * 1024, dimension_semantics=("arbitrary",)
        ),
        name="attend",
    )(q_all, found, key_page_scale.T, value_page_scale.T, k_rows, v_rows)

    columns = out_weight.shape[1] // parts
    return pl.pallas_call(
        functools.partial(project_kernel, sources, parts, heads),
        out_shape=jax.ShapeDtypeStruct((requests, columns), jnp.bfloat16),
        in_specs=[vmem, pl.BlockSpec(memory_space=pl.ANY)],
        out_specs=vmem,
        scratch_shapes=[
            pltpu.VMEM(out_weight.shape, jnp.bfloat16),
            pltpu.VMEM((sources, rows_here, width + LANES), jnp.bfloat16),
            pltpu.VMEM((rows_here, width), jnp.bfloat16),
            pltpu.VMEM((requests, width), jnp.bfloat16),
            pltpu.VMEM((parts, requests, columns), jnp.bfloat16),
            pltpu.VMEM((parts - 1, requests, columns), jnp.bfloat16),
            dma,
        ]
        + [dma((sources - 1,))] * 4
        + [dma((parts - 1,))] * 2,
        compiler_params=pltpu.CompilerParams(
            collective_id=1, has_side_effects=True, vmem_limit_bytes=63 * 1024 * 1024
        ),
        name="project",
    )(partial_sums, out_weight)


def solution(mesh):
    in_specs = (
        P("req", "head", None),
        P("req", None, "head", None),
        P("req", None, "head", None),
        P("req", "head"),
        P("req", "head"),
        P("req"),
        P("req", None),
        P("head", "req"),
    )
    out_specs = P(None, ("req", "head"))
    return jax.shard_map(
        on_device, mesh=mesh, in_specs=in_specs, out_specs=out_specs, check_vma=False
    )
```
